128 devices in a mesh: tm: 128 (over x, y, z, core).
Axes of the slice: x: 4, y: 4, z: 4, core: 2. Of those that a mesh axis runs over, the one named last changes fastest.
Arguments:
- stream: bfloat16 [262144, 64], P('tm'), may hold values from -6 to 6
- w_in: bfloat16 [64, 256], replicated, may hold values from -0.75 to 0.75
- w_conv: bfloat16 [4, 2, 256, 512], replicated, may hold values from -0.25 to 0.25
- w_residual: bfloat16 [3, 256, 256], replicated, may hold values from -0.375 to 0.375
- w_skip: bfloat16 [4, 256, 256], replicated, may hold values from -0.375 to 0.375
- w_out: bfloat16 [256, 64], replicated, may hold values from -0.375 to 0.375
- grad_pred: bfloat16 [262144, 64], P('tm'), may hold values from -0.01171875 to 0.01171875
Outputs:
- prediction: bfloat16 [262144, 64], P('tm')
- grad_w_in: float32 [64, 256], replicated
- grad_w_conv: float32 [4, 2, 256, 512], replicated
- grad_w_residual: float32 [3, 256, 256], replicated
- grad_w_skip: float32 [4, 256, 256], replicated
- grad_w_out: float32 [256, 64], replicated
The draws below stay inside these ranges and needn't reach their ends.
All inputs are finite; a program needn't handle non-finite values.
Results may differ from the reference program's by a relative error of at most 0.012.
Values may be sent and summed in bfloat16 or wider, within the bound.
No kernel may reach another device: no remote copies, remote signals or barrier semaphores. Data moves between devices by JAX's collectives and lax.ppermute only.
A program may use at most 128 MiB of HBM per device.

```python
import jax
import jax.numpy as jnp

FEAT = 64
RES = 256
GATE = 512
SKIP = 256
LAYERS = 4
TOK_DEV = 2048
TOKENS = 262144


def block_scale(stream_key, shape, split, low, top_value):
    loudness, own = 1.0, jax.random.fold_in(stream_key, 6)
    for axis_at, blocks in split:
        draws = jnp.exp(jax.random.uniform(jax.random.fold_in(own, axis_at), (blocks,), jnp.float32, low / len(split), top_value / len(split)))
        loudness = loudness * jnp.repeat(draws, shape[axis_at] // blocks).reshape([-1 if axis == axis_at else 1 for axis in range(len(shape))])
    return loudness


def centred(stream_key, shape, scale, most, split=(), held_as=jnp.bfloat16):
    result = jax.random.normal(stream_key, shape, jnp.float32) * scale
    if len(split) > 0:
        result = block_scale(stream_key, shape, split, -0.22, 0.18) * result
    return jnp.clip(result, min=-most, max=most).astype(held_as)


def setup_inputs(seed: int = 0) -> dict:
    seeds = jax.random.split(jax.random.key(seed), 8)
    return {
        "stream": centred(seeds[0], (TOKENS, FEAT), 1.0, 6.0, ((0, 128),)),
        "w_in": centred(seeds[1], (FEAT, RES), FEAT ** -0.5, 0.75),
        "w_conv": centred(seeds[2], (LAYERS, 2, RES, GATE), (2 * RES) ** -0.5, 0.25),
        "w_residual": centred(seeds[3], (LAYERS - 1, RES, RES), RES ** -0.5, 0.375),
        "w_skip": centred(seeds[4], (LAYERS, RES, SKIP), RES ** -0.5, 0.375),
        "w_out": centred(seeds[5], (SKIP, FEAT), SKIP ** -0.5, 0.375),
        "grad_pred": centred(seeds[6], (TOKENS, FEAT), (TOKENS ** -0.5), 0.01171875, ((0, 128),)),
    }


def lag_rows(h, dist):
    return jnp.concatenate([jnp.zeros((dist, h.shape[1]), h.dtype), h[:h.shape[0] - dist]], axis=0)


def unlag_rows(moved, dist):
    return jnp.concatenate([moved[dist:], jnp.zeros((dist, moved.shape[1]), moved.dtype)], axis=0)


def tdot(left, right):
    return jnp.dot(left.T, right, preferred_element_type=jnp.float32)


def reference(stream, w_in, w_conv, w_residual, w_skip, w_out, grad_pred):
    width = w_in.shape[1]
    h = jnp.dot(stream, w_in, preferred_element_type=jnp.float32).astype(jnp.bfloat16)
    skip = jnp.zeros((stream.shape[0], w_skip.shape[2]), jnp.float32)
    saved = []
    for layer in range(LAYERS):
        dist = TOK_DEV * 2 ** layer // 4
        lagged = lag_rows(h, dist)
        z = jnp.dot(lagged, w_conv[layer, 0], preferred_element_type=jnp.float32) + jnp.dot(h, w_conv[layer, 1], preferred_element_type=jnp.float32)
        gated = (jnp.tanh(z[:, :width]) * jax.nn.sigmoid(z[:, width:])).astype(jnp.bfloat16)
        skip = skip + jnp.dot(gated, w_skip[layer], preferred_element_type=jnp.float32)
        saved.append((h, lagged, z, gated))
        if layer < LAYERS - 1:
            h = (h.astype(jnp.float32) + jnp.dot(gated, w_residual[layer], preferred_element_type=jnp.float32)).astype(jnp.bfloat16)
    sig_skip = jax.nn.sigmoid(skip)
    active = (skip * sig_skip).astype(jnp.bfloat16)
    prediction = jnp.dot(active, w_out, preferred_element_type=jnp.float32).astype(jnp.bfloat16)
    grad_w_out = tdot(active, grad_pred)
    dact = jnp.dot(grad_pred, w_out.T, preferred_element_type=jnp.float32)
    dskip = (dact * sig_skip * (1.0 + skip * (1.0 - sig_skip))).astype(jnp.bfloat16)
    grad_conv = [None] * LAYERS
    grad_res = [None] * (LAYERS - 1)
    grad_skip = [None] * LAYERS
    dh = None
    for layer in reversed(range(LAYERS)):
        dist = TOK_DEV * 2 ** layer // 4
        h_l, lagged, z, gated = saved[layer]
        dg = jnp.dot(dskip, w_skip[layer].T, preferred_element_type=jnp.float32)
        grad_skip[layer] = tdot(gated, dskip)
        if layer < LAYERS - 1:
            dh_b = dh.astype(jnp.bfloat16)
            dg = dg + jnp.dot(dh_b, w_residual[layer].T, preferred_element_type=jnp.float32)
            grad_res[layer] = tdot(gated, dh_b)
        tanh_part = jnp.tanh(z[:, :width])
        sig_part = jax.nn.sigmoid(z[:, width:])
        dz = jnp.concatenate([dg * sig_part * (1.0 - tanh_part * tanh_part), dg * tanh_part * sig_part * (1.0 - sig_part)], axis=1).astype(jnp.bfloat16)
        grad_conv[layer] = jnp.stack([tdot(lagged, dz), tdot(h_l, dz)])
        new_dh = jnp.dot(dz, w_conv[layer, 1].T, preferred_element_type=jnp.float32) + unlag_rows(jnp.dot(dz, w_conv[layer, 0].T, preferred_element_type=jnp.float32), dist)
        if layer < LAYERS - 1:
            new_dh = new_dh + dh
        dh = new_dh
    grad_w_in = tdot(stream, dh.astype(jnp.bfloat16))
    return (prediction, grad_w_in, jnp.stack(grad_conv), jnp.stack(grad_res), jnp.stack(grad_skip), grad_w_out)
```

```python
import jax
import jax.numpy as jnp
from jax import lax
from jax.sharding import Mesh, PartitionSpec as P

CHIPS = ("x", "y", "z")
ALL = ("x", "y", "z", "c")
BF = jnp.bfloat16
F32 = jnp.float32


def tdot(left, right):
    return lax.dot_general(
        left, right, (((0,), (0,)), ((), ())), preferred_element_type=jnp.float32
    )


def lag_rows(h, dist):
    return jnp.concatenate([jnp.zeros((dist, h.shape[1]), h.dtype), h[: h.shape[0] - dist]], axis=0)


def unlag_rows(moved, dist):
    return jnp.concatenate([moved[dist:], jnp.zeros((dist, moved.shape[1]), moved.dtype)], axis=0)


def local_step(stream, w_in, w_conv, w_residual, w_skip, w_out, grad_pred, step):
    width = w_in.shape[1]
    layers = w_conv.shape[0]
    h = jnp.dot(stream, w_in, preferred_element_type=F32).astype(BF)
    skip = jnp.zeros((stream.shape[0], w_skip.shape[2]), F32)
    saved = []
    for layer in range(layers):
        lagged = lag_rows(h, step * 2**layer)
        z = jnp.dot(lagged, w_conv[layer, 0], preferred_element_type=F32) + jnp.dot(
            h, w_conv[layer, 1], preferred_element_type=F32
        )
        gated = (jnp.tanh(z[:, :width]) * jax.nn.sigmoid(z[:, width:])).astype(BF)
        skip = skip + jnp.dot(gated, w_skip[layer], preferred_element_type=F32)
        saved.append((h, lagged, z, gated))
        if layer < layers - 1:
            h = (
                h.astype(F32) + jnp.dot(gated, w_residual[layer], preferred_element_type=F32)
            ).astype(BF)
    sig_skip = jax.nn.sigmoid(skip)
    active = (skip * sig_skip).astype(BF)
    prediction = jnp.dot(active, w_out, preferred_element_type=F32).astype(BF)
    g_out = tdot(active, grad_pred)
    dact = jnp.dot(grad_pred, w_out.T, preferred_element_type=F32)
    dskip = (dact * sig_skip * (1.0 + skip * (1.0 - sig_skip))).astype(BF)
    g_conv = [None] * layers
    g_res = [None] * (layers - 1)
    g_skip = [None] * layers
    dh = None
    for layer in reversed(range(layers)):
        h_l, lagged, z, gated = saved[layer]
        dg = jnp.dot(dskip, w_skip[layer].T, preferred_element_type=F32)
        g_skip[layer] = tdot(gated, dskip)
        if layer < layers - 1:
            dh_b = dh.astype(BF)
            dg = dg + jnp.dot(dh_b, w_residual[layer].T, preferred_element_type=F32)
            g_res[layer] = tdot(gated, dh_b)
        a = jnp.tanh(z[:, :width])
        b = jax.nn.sigmoid(z[:, width:])
        dz = jnp.concatenate([dg * b * (1.0 - a * a), dg * a * b * (1.0 - b)], axis=1).astype(BF)
        g_conv[layer] = (tdot(lagged, dz), tdot(h_l, dz))
        new_dh = jnp.dot(dz, w_conv[layer, 1].T, preferred_element_type=F32) + unlag_rows(
            jnp.dot(dz, w_conv[layer, 0].T, preferred_element_type=F32), step * 2**layer
        )
        dh = new_dh if dh is None else new_dh + dh
    g_in = tdot(stream, dh.astype(BF))
    return prediction, g_in, g_conv, g_res, g_skip, g_out


def slabs(g):
    return [g[:, at : at + 128] for at in range(0, g.shape[1], 128)]


def unslab(flat, rows, cols):
    n = cols // 128
    return jnp.concatenate([flat[k * rows : (k + 1) * rows] for k in range(n)], axis=1)


def body(stream, w_in, w_conv, w_residual, w_skip, w_out, grad_pred):
    feat, width = w_in.shape
    rows = stream.shape[0]
    layers = w_conv.shape[0]
    gate = w_conv.shape[3]
    skip_width = w_skip.shape[2]
    chips = lax.axis_size(CHIPS)
    cores = lax.axis_size("c")
    devices = chips * cores
    smallest = rows // 4
    own = smallest // devices
    per = rows // devices
    both = jnp.concatenate([stream, grad_pred], axis=1)
    sent = both.reshape(per, devices, 2 * feat).transpose(1, 0, 2)
    got = lax.all_to_all(sent, ALL, 0, 0).reshape(rows, 2 * feat)
    prediction, g_in, g_conv, g_res, g_skip, g_out = local_step(
        got[:, :feat], w_in, w_conv, w_residual, w_skip, w_out, got[:, feat:], own
    )
    pieces = []
    for pair in g_conv:
        for g in pair:
            pieces += slabs(g)
    for g in g_skip:
        pieces += slabs(g)
    for g in g_res:
        pieces += slabs(g)
    pieces += slabs(g_in)
    half = width // 2
    pieces.append(jnp.concatenate([g_out[:half], g_out[half:]], axis=1))
    filled = sum(p.shape[0] for p in pieces)
    part = -(-filled // (devices * 16)) * 16
    pieces.append(jnp.zeros((part * devices - filled, 128), F32))
    flat = jnp.concatenate(pieces, axis=0).astype(BF).reshape(cores, chips, part, 128)
    pred = prediction.reshape(chips, cores, 2, per // 2, feat)
    pred = jnp.concatenate([pred[:, :, 0], pred[:, :, 1]], axis=-1).transpose(1, 0, 2, 3)
    mine = lax.axis_index("c")
    other = 1 - mine
    swap = [(0, 1), (1, 0)]
    joined = jnp.concatenate([flat, pred], axis=2)
    away = lax.ppermute(lax.dynamic_index_in_dim(joined, other, 0, keepdims=False), "c", swap)
    kept = lax.dynamic_index_in_dim(joined, mine, 0, keepdims=False)
    summed = (kept[:, :part].astype(F32) + away[:, :part].astype(F32)).astype(BF)
    from0 = jnp.where(mine == 0, kept[:, part:], away[:, part:])
    from1 = jnp.where(mine == 0, away[:, part:], kept[:, part:])
    out = lax.all_to_all(jnp.concatenate([summed, from0, from1], axis=1), CHIPS, 0, 0)
    total = jnp.sum(out[:, :part].astype(F32), axis=0).astype(BF)
    pred = out[:, part:].reshape(chips, cores, per // 2, 2, feat)
    pred = pred.transpose(3, 2, 0, 1, 4).reshape(rows, feat)
    spread = lax.all_to_all(jnp.broadcast_to(total[None], (chips, part, 128)), CHIPS, 0, 0)
    theirs = lax.ppermute(spread, "c", swap)
    low = jnp.where(mine == 0, spread, theirs)
    high = jnp.where(mine == 0, theirs, spread)
    flat = jnp.concatenate([low, high], axis=0).reshape(devices * part, 128)
    at = 0

    def take(r, c):
        nonlocal at
        n = r * c // 128
        piece = unslab(flat[at : at + n], r, c).astype(F32)
        at += n
        return piece

    o_conv = jnp.stack([jnp.stack([take(width, gate) for _ in range(2)]) for _ in range(layers)])
    o_skip = jnp.stack([take(width, skip_width) for _ in range(layers)])
    o_res = jnp.stack([take(width, width) for _ in range(layers - 1)])
    o_in = take(feat, width)
    packed = flat[at : at + half].astype(F32)
    o_out = jnp.concatenate([packed[:, :feat], packed[:, feat:]], axis=0)
    return pred, o_in, o_conv, o_res, o_skip, o_out


def solution(mesh):
    grid = Mesh(mesh.devices.reshape(4, 4, 4, 2), ALL)
    placed = (P(ALL, None), P(), P(), P(), P(), P(), P(ALL, None))
    return jax.shard_map(
        body,
        mesh=grid,
        in_specs=placed,
        out_specs=(P(ALL, None), P(), P(), P(), P(), P()),
        check_vma=False,
    )
```

```python
import functools
import jax
import jax.numpy as jnp
from jax import lax
from jax.experimental import pallas as pl
from jax.experimental.pallas import tpu as pltpu
from jax.sharding import Mesh, PartitionSpec as P

CHIPS = ("x", "y", "z")
ALL = ("x", "y", "z", "c")
BF = jnp.bfloat16
F32 = jnp.float32
LANES = 128
TILE = 16
GROUPS = 4
CHUNK = 512


def dot(left, right):
    return jnp.dot(left, right, preferred_element_type=F32)


def dot_bt(left, right):
    return lax.dot_general(left, right, (((1,), (1,)), ((), ())), preferred_element_type=F32)


def dot_at(left, right):
    return lax.dot_general(left, right, (((0,), (0,)), ((), ())), preferred_element_type=F32)


def up4(v):
    flat = v.reshape(-1, LANES)
    return pltpu.roll(flat, 4, 0).reshape(v.shape)


def down4(v):
    flat = v.reshape(-1, LANES)
    return pltpu.roll(flat, flat.shape[0] - 4, 0).reshape(v.shape)


def low_rows(shape):
    return lax.broadcasted_iota(jnp.int32, shape, len(shape) - 2) < 4


def step_kernel(
    mine_ref, got, w_first, w_conv, w_res, w_skip, w_wide, joined,
    xs, h0, h1, h2, h3, p_all, q_all, g_all, act, sd, dh, dz, acc, acc_sr, acc_io,
    *, layers, width, part, feat,
):
    rows = xs.shape[0]
    chunks = rows // CHUNK
    tiles = CHUNK // (TILE * GROUPS)
    hs = (h0, h1, h2, h3)
    mine = mine_ref[0]
    slots = (mine, 1 - mine)
    half_rows = joined.shape[1] * part
    top = h0.shape[0] - rows

    def at(c, offset=0):
        return pl.ds(pl.multiple_of(c * CHUNK + offset, TILE), CHUNK)

    def loop(fn):
        def step(c, carry):
            fn(c)
            return carry

        lax.fori_loop(0, chunks, step, 0)

    def put(row, value):
        n, done = value.shape[0], 0
        while done < n:
            half, inside = divmod(row + done, half_rows)
            chip, low = divmod(inside, part)
            take = min(part - low, n - done)
            joined[slots[half], chip, low : low + take, :] = value[done : done + take]
            done += take

    def put_slabs(row, value):
        for lane in range(0, value.shape[1], LANES):
            put(row, value[:, lane : lane + LANES].astype(BF))
            row += value.shape[0]
        return row

    def regroup(c):
        g = [got[s, pl.ds(c * tiles, tiles)].astype(F32).reshape(tiles, 2, 8, LANES) for s in range(4)]
        low = low_rows(g[0].shape)
        even = [jnp.where(low, g[2 * k], up4(g[2 * k + 1])) for k in range(2)]
        odd = [jnp.where(low, down4(g[2 * k]), g[2 * k + 1]) for k in range(2)]
        whole = jnp.stack([jnp.stack(even, axis=2), jnp.stack(odd, axis=2)], axis=2)
        x = whole.reshape(CHUNK, LANES).astype(BF)
        xs[at(c)] = x
        h0[at(c, top)] = dot(x, w_first[:, :width]).astype(BF)

    loop(regroup)

    def wrapped(tail, by):
        v = tail.astype(F32)
        n = v.shape[0]
        v = pltpu.roll(v, by % n, 0)
        row = lax.broadcasted_iota(jnp.int32, v.shape, 0) % TILE
        keep = row >= by if by > 0 else row < TILE + by
        return jnp.where(keep, v, 0.0).astype(BF)

    for layer in range(layers):
        h = hs[layer]
        lag = TILE * 2**layer
        h[top - lag : top] = wrapped(h[top + rows - lag :], 4)
        w = w_conv[layer].reshape(2 * width, 2 * width)

        def forward(c, layer=layer, h=h, lag=lag):
            here = h[at(c, top)]
            z = dot(h[at(c, top - lag)], w_conv[layer, 0]) + dot(here, w_conv[layer, 1])
            a = jnp.tanh(z[:, :width])
            b = 0.5 * jnp.tanh(0.5 * z[:, width:]) + 0.5
            g = a * b
            p_all[layer, at(c)] = b - a * g
            q_all[layer, at(c)] = g - g * b
            gated = g.astype(BF)
            g_all[at(c), layer * width : (layer + 1) * width] = gated
            if layer < layers - 1:
                hs[layer + 1][at(c, top)] = (here.astype(F32) + dot(gated, w_res[layer])).astype(BF)

        loop(forward)

    acc_io[...] = jnp.zeros(acc_io.shape, F32)

    def head(c):
        skip = dot(g_all[at(c)], w_skip[...].reshape(layers * width, width))
        s = 0.5 * jnp.tanh(0.5 * skip) + 0.5
        active = (skip * s).astype(BF)
        x = xs[at(c)]
        sd[at(c), :width] = (dot(x, w_first[:, width:]) * s * (1.0 + skip * (1.0 - s))).astype(BF)
        acc_io[...] += dot_at(x, active)
        both = dot(active, w_wide[...])
        pa = both[:, :LANES].reshape(tiles, 4, 2, 8, LANES)
        pb = both[:, LANES:].reshape(tiles, 4, 2, 8, LANES)
        u = pa[:, 0] + pb[:, 2]
        v = pa[:, 1] + pb[:, 3]
        low = low_rows(u.shape)
        even = jnp.where(low, u, up4(v))
        odd = jnp.where(low, down4(u), v)
        for s in range(GROUPS):
            from_seg = (even, odd)[s % 2][:, s // 2].reshape(tiles // 2, 2, 8, LANES)
            for core in range(2):
                rows8 = from_seg[:, core]
                tile = jnp.concatenate(
                    [jnp.where(mine == 0, rows8, 0.0), jnp.where(mine == 1, rows8, 0.0)], axis=1
                )
                chip = pl.ds(s * (joined.shape[1] // GROUPS) + c * (tiles // 2), tiles // 2)
                joined[slots[core], chip, part:, :] = tile.astype(BF)

    loop(head)
    at_conv = 0
    at_skip = layers * 2 * width * 2 * width // LANES
    at_res = at_skip + layers * width * width // LANES
    at_in = at_res + (layers - 1) * width * width // LANES
    at_out = at_in + feat * width // LANES
    end = put_slabs(at_out, acc_io[feat:, :])
    spare = joined.shape[0] * half_rows - end
    put(end, jnp.zeros((spare, LANES), BF))

    for layer in reversed(range(layers)):
        h = hs[layer]
        lag = TILE * 2**layer
        last = layer == layers - 1
        acc_sr[...] = jnp.zeros(acc_sr.shape, F32)
        acc[...] = jnp.zeros(acc.shape, F32)

        def gate(c, layer=layer, last=last):
            dg = dot_bt(sd[at(c), :width], w_skip[layer])
            if not last:
                dg = dg + dot_bt(sd[at(c), width:], w_res[layer])
            dz[at(c), :width] = (dg * p_all[layer, at(c)]).astype(BF)
            dz[at(c), width:] = (dg * q_all[layer, at(c)]).astype(BF)
            gated = g_all[at(c), layer * width : (layer + 1) * width]
            if last:
                acc_sr[:, :width] += dot_at(gated, sd[at(c), :width])
            else:
                acc_sr[...] += dot_at(gated, sd[at(c)])

        loop(gate)
        dz[rows : rows + lag] = wrapped(dz[:lag], -4)

        def taps(c, layer=layer, last=last, h=h, lag=lag):
            later = dz[at(c, lag)]
            here = dz[at(c)]
            grown = dot_bt(later, w_conv[layer, 0]) + dot_bt(here, w_conv[layer, 1])
            if not last:
                grown = grown + dh[at(c)]
            dh[at(c)] = grown
            sd[at(c), width:] = grown.astype(BF)
            x = h[at(c, top)]
            acc[...] += dot_at(x, jnp.concatenate([later, here], axis=1))

        loop(taps)
        row = put_slabs(at_conv + layer * 4 * width * width // LANES, acc[:, : 2 * width])
        put_slabs(row, acc[:, 2 * width :])
        put_slabs(at_skip + layer * width * width // LANES, acc_sr[:, :width])
        if not last:
            put_slabs(at_res + layer * width * width // LANES, acc_sr[:, width:])

    acc_io[...] = jnp.zeros(acc_io.shape, F32)

    def first(c):
        acc_io[...] += dot_at(xs[at(c)], sd[at(c), width:])

    loop(first)
    put_slabs(at_in, acc_io[:feat, :])


def local_step(mine, got, w_in, w_conv, w_res, w_skip, w_out, chips, part, interpret=False):
    feat, width = w_in.shape
    layers = w_conv.shape[0]
    rows = got.shape[0] * got.shape[1]
    none = jnp.zeros((feat, width), BF)
    w_first = jnp.concatenate(
        [jnp.concatenate([w_in, none], axis=0), jnp.concatenate([none, w_out.T], axis=0)], axis=1
    )
    gap = jnp.zeros((width, feat), BF)
    w_wide = jnp.concatenate([w_out, gap, gap, w_out], axis=1)
    pad = TILE * 2 ** (layers - 1)
    vmem = pl.BlockSpec(memory_space=pltpu.VMEM)
    flops = 2 * rows * width * (layers * (3 * 4 * width + 3 * 2 * width))
    return pl.pallas_call(
        functools.partial(step_kernel, layers=layers, width=width, part=part, feat=feat),
        out_shape=jax.ShapeDtypeStruct((2, chips, part + TILE, LANES), BF),
        in_specs=[pl.BlockSpec(memory_space=pltpu.SMEM)] + [vmem] * 6,
        out_specs=vmem,
        scratch_shapes=[pltpu.VMEM((rows, LANES), BF)]
        + [pltpu.VMEM((rows + pad, width), BF)] * layers
        + [
            pltpu.VMEM((layers, rows, width), F32),
            pltpu.VMEM((layers, rows, width), F32),
            pltpu.VMEM((rows, layers * width), BF),
            pltpu.VMEM((rows, width), BF),
            pltpu.VMEM((rows, 2 * width), BF),
            pltpu.VMEM((rows, width), F32),
            pltpu.VMEM((rows + pad, 2 * width), BF),
            pltpu.VMEM((width, 4 * width), F32),
            pltpu.VMEM((width, 2 * width), F32),
            pltpu.VMEM((LANES, width), F32),
        ],
        compiler_params=pltpu.CompilerParams(vmem_limit_bytes=60000 * 1024),
        cost_estimate=pl.CostEstimate(flops=flops, transcendentals=rows * width * 2 * layers, bytes_accessed=2**23),
        interpret=interpret,
        name="residue_step",
    )(mine, got.reshape(GROUPS, -1, TILE, LANES), w_first, w_conv, w_res, w_skip, w_wide)


def unslab(flat, rows, cols):
    n = cols // LANES
    return jnp.concatenate([flat[k * rows : (k + 1) * rows] for k in range(n)], axis=1)


def body(stream, w_in, w_conv, w_residual, w_skip, w_out, grad_pred):
    feat, width = w_in.shape
    rows = stream.shape[0]
    layers = w_conv.shape[0]
    gate = w_conv.shape[3]
    skip_width = w_skip.shape[2]
    chips = lax.axis_size(CHIPS)
    cores = lax.axis_size("c")
    devices = chips * cores
    per = rows // devices
    both = jnp.concatenate([stream, grad_pred], axis=1)
    sent = both.reshape(per, devices, 2 * feat).transpose(1, 0, 2)
    got = lax.all_to_all(sent, ALL, 0, 0)
    mine = lax.axis_index("c")
    swap = [(0, 1), (1, 0)]
    filled = (w_conv.size + w_residual.size + w_skip.size + w_in.size + w_out.size) // LANES
    part = -(-filled // (devices * TILE)) * TILE
    joined = local_step(mine[None], got, w_in, w_conv, w_residual, w_skip, w_out, chips, part)
    away = lax.ppermute(joined[1], "c", swap)
    summed = (joined[0].astype(F32) + away.astype(F32)).astype(BF)
    out = lax.all_to_all(summed, CHIPS, 0, 0)
    total = jnp.sum(out[:, :part].astype(F32), axis=0).astype(BF)
    pred = out[:, part:].reshape(chips, cores, per // 2, 2, feat)
    pred = pred.transpose(3, 2, 0, 1, 4).reshape(rows, feat)
    spread = lax.all_to_all(jnp.broadcast_to(total[None], (chips, part, LANES)), CHIPS, 0, 0)
    theirs = lax.ppermute(spread, "c", swap)
    low = jnp.where(mine == 0, spread, theirs)
    high = jnp.where(mine == 0, theirs, spread)
    flat = jnp.concatenate([low, high], axis=0).reshape(devices * part, LANES)
    at = 0

    def take(r, c):
        nonlocal at
        n = r * c // LANES
        piece = unslab(flat[at : at + n], r, c).astype(F32)
        at += n
        return piece

    o_conv = jnp.stack([jnp.stack([take(width, gate) for _ in range(2)]) for _ in range(layers)])
    o_skip = jnp.stack([take(width, skip_width) for _ in range(layers)])
    o_res = jnp.stack([take(width, width) for _ in range(layers - 1)])
    o_in = take(feat, width)
    o_out = take(feat, skip_width).T
    return pred, o_in, o_conv, o_res, o_skip, o_out


def solution(mesh):
    grid = Mesh(mesh.devices.reshape(4, 4, 4, 2), ALL)
    placed = (P(ALL, None), P(), P(), P(), P(), P(), P(ALL, None))
    return jax.shard_map(
        body,
        mesh=grid,
        in_specs=placed,
        out_specs=(P(ALL, None), P(), P(), P(), P(), P()),
        check_vma=False,
    )
```

```python
import functools
import jax
import jax.numpy as jnp
from jax import lax
from jax.experimental import pallas as pl
from jax.experimental.pallas import tpu as pltpu
from jax.sharding import Mesh, PartitionSpec as P

CHIPS = ("x", "y", "z")
ALL = ("x", "y", "z", "c")
BF = jnp.bfloat16
F32 = jnp.float32
LANES = 128
TILE = 16
GROUPS = 4
VMEM = pl.BlockSpec(memory_space=pltpu.VMEM)
SMEM = pl.BlockSpec(memory_space=pltpu.SMEM)
ANY = pl.BlockSpec(memory_space=pl.ANY)
HBM = pl.BlockSpec(memory_space=pltpu.HBM)


def grant(mib):
    return pltpu.CompilerParams(vmem_limit_bytes=mib * 2**20)


def dot(left, right):
    return jnp.dot(left, right, preferred_element_type=F32)


def dot_bt(left, right):
    return lax.dot_general(left, right, (((1,), (1,)), ((), ())), preferred_element_type=F32)


def dot_at(left, right):
    return lax.dot_general(left, right, (((0,), (0,)), ((), ())), preferred_element_type=F32)


def merge(left, right):
    def shift(v, by):
        flat = v.reshape(-1, LANES)
        return pltpu.roll(flat, by % flat.shape[0], 0).reshape(v.shape)

    low = lax.broadcasted_iota(jnp.int32, left.shape, left.ndim - 2) < 4
    return jnp.where(low, left, shift(right, 4)), jnp.where(low, shift(left, -4), right)


def regroup_kernel(stream_t, grad_t, sent, both, sems):
    feat = stream_t.shape[0]
    copies = [
        pltpu.make_async_copy(stream_t, both.at[:feat], sems.at[0]),
        pltpu.make_async_copy(grad_t, both.at[feat:], sems.at[1]),
    ]
    for copy in copies:
        copy.start()
    for copy in copies:
        copy.wait()
    x = both[...].astype(F32).T
    devices = sent.shape[0]
    x = x.reshape(4, devices // 2, 8, LANES)
    halves = []
    for k in range(2):
        even, odd = merge(x[2 * k], x[2 * k + 1])
        halves.append(jnp.stack([even, odd], axis=1))
    sent[...] = jnp.stack(halves, axis=2).reshape(sent.shape).astype(BF)


def step_kernel(
    mine_ref, got, w_in_at, w_conv_at, w_res_at, w_skip_at, w_out_at, keep_out, send_out,
    w_in, w_conv, w_res, w_skip, w_out_t, w_first, w_wide_t, xs, h0, h1, h2, h3, p_all, q_all, g_all, sd, dh, dz, joined, sems,
    *, layers, width, part, feat,
):
    rows = xs.shape[0]
    steps = rows // (TILE * GROUPS)
    hs = (h0, h1, h2, h3)
    mine = mine_ref[0]
    slots = (mine, 1 - mine)
    half_rows = joined.shape[1] * part
    top = h0.shape[0] - rows

    def put(row, value):
        n, done = value.shape[0], 0
        while done < n:
            half, inside = divmod(row + done, half_rows)
            chip, low = divmod(inside, part)
            take = min(part - low, n - done)
            joined[slots[half], chip, low : low + take, :] = value[done : done + take]
            done += take

    def put_slabs(row, value):
        for lane in range(0, value.shape[1], LANES):
            put(row, value[:, lane : lane + LANES].astype(BF))
            row += value.shape[0]
        return row

    def wrapped(tail, by):
        v = tail.astype(F32)
        v = pltpu.roll(v, by % v.shape[0], 0)
        row = lax.broadcasted_iota(jnp.int32, v.shape, 0) % TILE
        keep = row >= by if by > 0 else row < TILE + by
        return jnp.where(keep, v, 0.0).astype(BF)

    def fetch(source, to, at):
        copy = pltpu.make_async_copy(source, to, sems.at[at])
        copy.start()
        return copy

    ends = [fetch(w_in_at, w_in, 2), fetch(w_out_at, w_out_t, 3)]
    conv_copies = [fetch(w_conv_at.at[i], w_conv.at[i], 4 + i) for i in range(layers)]
    res_copy = fetch(w_res_at, w_res, 4 + layers)
    skip_copy = fetch(w_skip_at, w_skip, 5 + layers)

    g = [got[s].astype(F32).reshape(steps, 2, 8, LANES) for s in range(GROUPS)]
    pairs = [merge(g[2 * k], g[2 * k + 1]) for k in range(2)]
    even = jnp.stack([pairs[0][0], pairs[1][0]], axis=2)
    odd = jnp.stack([pairs[0][1], pairs[1][1]], axis=2)
    xs[...] = jnp.stack([even, odd], axis=2).reshape(rows, LANES).astype(BF)
    for copy in ends:
        copy.wait()
    none = jnp.zeros((feat, width), BF)
    w_first[:feat, :width] = w_in[...]
    w_first[feat:, :width] = none
    w_first[:feat, width:] = none
    w_first[feat:, width:] = w_out_t[...]
    w_wide_t[:feat, :] = w_out_t[...]
    w_wide_t[feat : 2 * feat, :] = none
    w_wide_t[2 * feat : 3 * feat, :] = none
    w_wide_t[3 * feat :, :] = w_out_t[...]
    h0[top:, :] = dot(xs[...], w_first[:, :width]).astype(BF)

    for layer in range(layers):
        h = hs[layer]
        lag = TILE * 2**layer
        h[top - lag : top] = wrapped(h[top + rows - lag :], 4)
        here = h[top:, :]
        conv_copies[layer].wait()
        if layer == 0:
            res_copy.wait()
        z = dot(h[top - lag : top - lag + rows, :], w_conv[layer, 0]) + dot(here, w_conv[layer, 1])
        a = jnp.tanh(z[:, :width])
        b = 0.5 * jnp.tanh(0.5 * z[:, width:]) + 0.5
        gate = a * b
        p_all[layer] = (b - a * gate).astype(BF)
        q_all[layer] = (gate - gate * b).astype(BF)
        gated = gate.astype(BF)
        g_all[:, layer * width : (layer + 1) * width] = gated
        if layer < layers - 1:
            hs[layer + 1][top:, :] = (here.astype(F32) + dot(gated, w_res[layer])).astype(BF)

    skip_copy.wait()
    skip = dot(g_all[...], w_skip[...].reshape(layers * width, width))
    s = 0.5 * jnp.tanh(0.5 * skip) + 0.5
    active = (skip * s).astype(BF)
    sd[:, :width] = (dot(xs[...], w_first[:, width:]) * s * (1.0 + skip * (1.0 - s))).astype(BF)
    both = dot_bt(active, w_wide_t[...])
    pa = both[:, :LANES].reshape(steps, 4, 2, 8, LANES)
    pb = both[:, LANES:].reshape(steps, 4, 2, 8, LANES)
    even, odd = merge(pa[:, 0] + pb[:, 2], pa[:, 1] + pb[:, 3])
    chips = joined.shape[1] // GROUPS
    for seg in range(GROUPS):
        from_seg = (even, odd)[seg % 2][:, seg // 2].reshape(chips, 2, 8, LANES)
        for core in range(2):
            rows8 = from_seg[:, core]
            tile = jnp.concatenate(
                [jnp.where(mine == 0, rows8, 0.0), jnp.where(mine == 1, rows8, 0.0)], axis=1
            )
            joined[slots[core], seg * chips : (seg + 1) * chips, part:, :] = tile.astype(BF)

    at_skip = layers * 4 * width * width // LANES
    at_res = at_skip + layers * width * width // LANES
    at_in = at_res + (layers - 1) * width * width // LANES
    at_out = at_in + feat * width // LANES
    end = put_slabs(at_out, dot_at(xs[...], active)[feat:, :])
    put(end, jnp.zeros((joined.shape[0] * half_rows - end, LANES), BF))

    for layer in reversed(range(layers)):
        h = hs[layer]
        lag = TILE * 2**layer
        last = layer == layers - 1
        dg = dot_bt(sd[:, :width], w_skip[layer])
        if not last:
            dg = dg + dot_bt(sd[:, width:], w_res[layer])
        dz[:rows, :width] = (dg * p_all[layer].astype(F32)).astype(BF)
        dz[:rows, width:] = (dg * q_all[layer].astype(F32)).astype(BF)
        gated = g_all[:, layer * width : (layer + 1) * width]
        side = dot_at(gated, sd[:, :width] if last else sd[...])
        put_slabs(at_skip + layer * width * width // LANES, side[:, :width])
        if not last:
            put_slabs(at_res + layer * width * width // LANES, side[:, width:])
        dz[rows : rows + lag] = wrapped(dz[:lag], -4)
        later = dz[lag : lag + rows]
        here = dz[:rows]
        grown = dot_bt(later, w_conv[layer, 0]) + dot_bt(here, w_conv[layer, 1])
        if not last:
            grown = grown + dh[...]
        dh[...] = grown
        sd[:, width:] = grown.astype(BF)
        row = layer * 4 * width * width // LANES
        row = put_slabs(row, dot_at(h[top:, :], later))
        put_slabs(row, dot_at(h[top:, :], here))

    put_slabs(at_in, dot_at(xs[...], sd[:, width:])[:feat, :])
    send = pltpu.make_async_copy(joined.at[1], send_out, sems.at[0])
    keep = pltpu.make_async_copy(joined.at[0], keep_out, sems.at[1])
    send.start()
    keep.start()
    send.wait()
    keep.wait()


def local_step(mine, got, w_in, w_conv, w_res, w_skip, w_out, chips, part):
    feat, width = w_in.shape
    layers = w_conv.shape[0]
    rows = got.shape[0] * got.shape[1]
    pad = TILE * 2 ** (layers - 1)
    flops = 2 * rows * width * (layers * (3 * 4 * width + 3 * 2 * width))
    half = jax.ShapeDtypeStruct((chips, part + TILE, LANES), BF)
    return pl.pallas_call(
        functools.partial(step_kernel, layers=layers, width=width, part=part, feat=feat),
        out_shape=(half, half),
        in_specs=[SMEM, VMEM] + [HBM] * 5,
        out_specs=(ANY, ANY),
        scratch_shapes=[
            pltpu.VMEM(w_in.shape, BF),
            pltpu.VMEM(w_conv.shape, BF),
            pltpu.VMEM(w_res.shape, BF),
            pltpu.VMEM(w_skip.shape, BF),
            pltpu.VMEM(w_out.shape[::-1], BF),
            pltpu.VMEM((LANES, 2 * width), BF),
            pltpu.VMEM((2 * LANES, width), BF),
            pltpu.VMEM((rows, LANES), BF),
        ]
        + [pltpu.VMEM((rows + pad, width), BF)] * layers
        + [
            pltpu.VMEM((layers, rows, width), BF),
            pltpu.VMEM((layers, rows, width), BF),
            pltpu.VMEM((rows, layers * width), BF),
            pltpu.VMEM((rows, 2 * width), BF),
            pltpu.VMEM((rows, width), F32),
            pltpu.VMEM((rows + pad, 2 * width), BF),
            pltpu.VMEM((2, chips, part + TILE, LANES), BF),
            pltpu.SemaphoreType.DMA((6 + layers,)),
        ],
        compiler_params=grant(46),
        cost_estimate=pl.CostEstimate(
            flops=flops, transcendentals=rows * width * 2 * layers, bytes_accessed=2**23
        ),
        name="residue_step",
    )(
        mine,
        got.reshape(GROUPS, -1, TILE, LANES),
        *(pltpu.with_memory_space_constraint(w, pltpu.HBM) for w in (w_in, w_conv, w_res, w_skip, w_out.T)),
    )


def total_kernel(out, spread, pred_t, *, part):
    chips = out.shape[0]
    total = jnp.sum(out[:, :part, :].astype(F32), axis=0).astype(BF)
    for chip in range(chips):
        spread[chip] = total
    rows = out[:, part:, :].astype(F32).reshape(chips, 2, 8, LANES)
    span = chips * 8
    for k, piece in enumerate(merge(rows[:, 0], rows[:, 1])):
        turned = piece.reshape(span, LANES).T
        for half in range(2):
            at = (2 * half + k) * span
            pred_t[:, at : at + span] = turned[half * 64 : half * 64 + 64].astype(BF)


def unpack_kernel(
    mine_ref, spread, theirs, conv_out, res_out, skip_out, in_out, out_out,
    conv, res, skip, first, last, sems,
    *, part,
):
    here = mine_ref[0] == 0
    half_rows = spread.shape[0] * part
    copies = []

    def piece(row, n):
        got = []
        while n > 0:
            half, inside = divmod(row, half_rows)
            chip, low = divmod(inside, part)
            take = min(part - low, n)
            a, b = spread[chip, low : low + take, :], theirs[chip, low : low + take, :]
            got.append(jnp.where(here, a, b) if half == 0 else jnp.where(here, b, a))
            row, n = row + take, n - take
        return got

    def fill(row, to):
        rows, cols = to.shape
        for lane in range(0, cols, LANES):
            at = 0
            for got in piece(row, rows):
                to[at : at + got.shape[0], lane : lane + LANES] = got.astype(F32)
                at += got.shape[0]
            row += rows
        return row

    def leave(scratch, out):
        copy = pltpu.make_async_copy(scratch, out, sems.at[len(copies)])
        copy.start()
        copies.append(copy)

    row = 0
    for layer in range(conv.shape[0]):
        for tap in range(2):
            row = fill(row, conv.at[layer, tap])
        leave(conv.at[layer], conv_out.at[layer])
    for kind, out in ((skip, skip_out), (res, res_out)):
        for layer in range(kind.shape[0]):
            row = fill(row, kind.at[layer])
        leave(kind, out)
    for kind, out in ((first, in_out), (last, out_out)):
        row = fill(row, kind)
        leave(kind, out)
    for copy in copies:
        copy.wait()


def body(stream, w_in, w_conv, w_res, w_skip, w_out, grad_pred):
    feat, width = w_in.shape
    rows = stream.shape[0]
    chips = lax.axis_size(CHIPS)
    devices = chips * lax.axis_size("c")
    sent = pl.pallas_call(
        regroup_kernel,
        out_shape=jax.ShapeDtypeStruct((devices, TILE, LANES), BF),
        in_specs=[HBM] * 2,
        out_specs=VMEM,
        scratch_shapes=[pltpu.VMEM((2 * feat, rows), BF), pltpu.SemaphoreType.DMA((2,))],
        compiler_params=grant(8),
        name="regroup",
    )(*(pltpu.with_memory_space_constraint(x.T, pltpu.HBM) for x in (stream, grad_pred)))
    got = lax.all_to_all(sent, ALL, 0, 0)
    mine = lax.axis_index("c")[None]
    swap = [(0, 1), (1, 0)]
    filled = (w_conv.size + w_res.size + w_skip.size + w_in.size + w_out.size) // LANES
    part = -(-filled // (devices * TILE)) * TILE
    kept, sent = local_step(mine, got, w_in, w_conv, w_res, w_skip, w_out, chips, part)
    away = lax.ppermute(sent, "c", swap)
    summed = (kept.astype(F32) + away.astype(F32)).astype(BF)
    out = lax.all_to_all(summed, CHIPS, 0, 0)
    spread, pred_t = pl.pallas_call(
        functools.partial(total_kernel, part=part),
        out_shape=(
            jax.ShapeDtypeStruct((chips, part, LANES), BF),
            jax.ShapeDtypeStruct((feat, rows), BF),
        ),
        in_specs=[VMEM],
        out_specs=(VMEM, VMEM),
        compiler_params=grant(10),
        name="total",
    )(out)
    spread = lax.all_to_all(spread, CHIPS, 0, 0)
    theirs = lax.ppermute(spread, "c", swap)
    shapes = [w_conv.shape, w_res.shape, w_skip.shape, w_in.shape, w_out.shape[::-1]]
    o_conv, o_res, o_skip, o_in, o_out_t = pl.pallas_call(
        functools.partial(unpack_kernel, part=part),
        out_shape=tuple(jax.ShapeDtypeStruct(s, F32) for s in shapes),
        in_specs=[SMEM, VMEM, VMEM],
        out_specs=(ANY,) * 5,
        scratch_shapes=[pltpu.VMEM(s, F32) for s in shapes]
        + [pltpu.SemaphoreType.DMA((w_conv.shape[0] + 4,))],
        compiler_params=grant(12),
        name="unpack",
    )(mine, spread, theirs)
    return pred_t.T, o_in, o_conv, o_res, o_skip, o_out_t.T


def solution(mesh):
    grid = Mesh(mesh.devices.reshape(4, 4, 4, 2), ALL)
    placed = (P(ALL, None), P(), P(), P(), P(), P(), P(ALL, None))
    return jax.shard_map(
        body,
        mesh=grid,
        in_specs=placed,
        out_specs=(P(ALL, None), P(), P(), P(), P(), P()),
        check_vma=False,
    )
```

```python
import functools
import jax
import jax.numpy as jnp
from jax import lax
from jax.experimental import pallas as pl
from jax.experimental.pallas import tpu as pltpu
from jax.sharding import Mesh, PartitionSpec as P

CHIPS = ("x", "y", "z")
ALL = ("x", "y", "z", "c")
BF = jnp.bfloat16
F32 = jnp.float32
LANES = 128
TILE = 16
SPLIT = 4
GROUPS = 4
VMEM = pl.BlockSpec(memory_space=pltpu.VMEM)
SMEM = pl.BlockSpec(memory_space=pltpu.SMEM)
ANY = pl.BlockSpec(memory_space=pl.ANY)
HBM = pl.BlockSpec(memory_space=pltpu.HBM)


def grant(mib):
    return pltpu.CompilerParams(vmem_limit_bytes=mib * 2**20)


def dot(left, right):
    return jnp.dot(left, right, preferred_element_type=F32)


def dot_bt(left, right):
    return lax.dot_general(left, right, (((1,), (1,)), ((), ())), preferred_element_type=F32)


def dot_at(left, right):
    return lax.dot_general(left, right, (((0,), (0,)), ((), ())), preferred_element_type=F32)


def merge(left, right):
    def shift(v, by):
        flat = v.reshape(-1, LANES)
        return pltpu.roll(flat, by % flat.shape[0], 0).reshape(v.shape)

    low = lax.broadcasted_iota(jnp.int32, left.shape, left.ndim - 2) < 4
    return jnp.where(low, left, shift(right, 4)), jnp.where(low, shift(left, -4), right)


def regroup_kernel(stream_t, grad_t, sent, both, sems):
    feat = stream_t.shape[0]
    copies = [
        pltpu.make_async_copy(stream_t, both.at[:feat], sems.at[0]),
        pltpu.make_async_copy(grad_t, both.at[feat:], sems.at[1]),
    ]
    for copy in copies:
        copy.start()
    for copy in copies:
        copy.wait()
    x = both[...].astype(F32).T
    devices = sent.shape[0]
    x = x.reshape(4, devices // 2, 8, LANES)
    halves = []
    for k in range(2):
        even, odd = merge(x[2 * k], x[2 * k + 1])
        halves.append(jnp.stack([even, odd], axis=1))
    sent[...] = jnp.stack(halves, axis=2).reshape(sent.shape).astype(BF)


def step_kernel(
    mine_ref, got, w_in_at, w_conv_at, w_res_at, w_skip_at, w_out_at, keep_out, send_out,
    w_in, w_conv, w_res, w_skip, w_out_t, w_first, w_wide_t, xs, h0, h1, h2, h3, p_all, q_all, g_all, sd, dh, dz, joined, sems,
    *, layers, width, part, feat,
):
    rows = xs.shape[0]
    steps = rows // (TILE * GROUPS)
    hs = (h0, h1, h2, h3)
    mine = mine_ref[0]
    slots = (mine, 1 - mine)
    half_rows = joined.shape[1] * part
    top = h0.shape[0] - rows

    def put(row, value):
        n, done = value.shape[0], 0
        while done < n:
            half, inside = divmod(row + done, half_rows)
            chip, low = divmod(inside, part)
            take = min(part - low, n - done)
            joined[slots[half], chip, low : low + take, :] = value[done : done + take]
            done += take

    def put_slabs(row, value):
        for lane in range(0, value.shape[1], LANES):
            put(row, value[:, lane : lane + LANES].astype(BF))
            row += value.shape[0]
        return row

    def wrapped(tail, by):
        v = tail.astype(F32)
        v = pltpu.roll(v, by % v.shape[0], 0)
        row = lax.broadcasted_iota(jnp.int32, v.shape, 0) % TILE
        keep = row >= by if by > 0 else row < TILE + by
        return jnp.where(keep, v, 0.0).astype(BF)

    def fetch(source, to, at):
        copy = pltpu.make_async_copy(source, to, sems.at[at])
        copy.start()
        return copy

    ends = [fetch(w_in_at, w_in, 2), fetch(w_out_at, w_out_t, 3)]
    conv_copies = [fetch(w_conv_at.at[i], w_conv.at[i], 4 + i) for i in range(layers)]
    res_copy = fetch(w_res_at, w_res, 4 + layers)
    skip_copy = fetch(w_skip_at, w_skip, 5 + layers)

    g = [got[s].astype(F32).reshape(steps, 2, 8, LANES) for s in range(GROUPS)]
    pairs = [merge(g[2 * k], g[2 * k + 1]) for k in range(2)]
    even = jnp.stack([pairs[0][0], pairs[1][0]], axis=2)
    odd = jnp.stack([pairs[0][1], pairs[1][1]], axis=2)
    xs[...] = jnp.stack([even, odd], axis=2).reshape(rows, LANES).astype(BF)
    for copy in ends:
        copy.wait()
    none = jnp.zeros((feat, width), BF)
    w_first[:feat, :width] = w_in[...]
    w_first[feat:, :width] = none
    w_first[:feat, width:] = none
    w_first[feat:, width:] = w_out_t[...]
    w_wide_t[:feat, :] = w_out_t[...]
    w_wide_t[feat : 2 * feat, :] = none
    w_wide_t[2 * feat : 3 * feat, :] = none
    w_wide_t[3 * feat :, :] = w_out_t[...]
    h0[top:, :] = dot(xs[...], w_first[:, :width]).astype(BF)

    for layer in range(layers):
        h = hs[layer]
        lag = TILE * 2**layer
        h[top - lag : top] = wrapped(h[top + rows - lag :], 4)
        here = h[top:, :]
        conv_copies[layer].wait()
        if layer == 0:
            res_copy.wait()
        z = dot(h[top - lag : top - lag + rows, :], w_conv[layer, 0]) + dot(here, w_conv[layer, 1])
        a = jnp.tanh(z[:, :width])
        b = 0.5 * jnp.tanh(0.5 * z[:, width:]) + 0.5
        gate = a * b
        p_all[layer] = (b - a * gate).astype(BF)
        q_all[layer] = (gate - gate * b).astype(BF)
        gated = gate.astype(BF)
        g_all[:, layer * width : (layer + 1) * width] = gated
        if layer < layers - 1:
            hs[layer + 1][top:, :] = (here.astype(F32) + dot(gated, w_res[layer])).astype(BF)

    skip_copy.wait()
    skip = dot(g_all[...], w_skip[...].reshape(layers * width, width))
    s = 0.5 * jnp.tanh(0.5 * skip) + 0.5
    active = (skip * s).astype(BF)
    sd[:, :width] = (dot(xs[...], w_first[:, width:]) * s * (1.0 + skip * (1.0 - s))).astype(BF)
    both = dot_bt(active, w_wide_t[...])
    pa = both[:, :LANES].reshape(steps, 4, 2, 8, LANES)
    pb = both[:, LANES:].reshape(steps, 4, 2, 8, LANES)
    even, odd = merge(pa[:, 0] + pb[:, 2], pa[:, 1] + pb[:, 3])
    chips = joined.shape[1] // GROUPS
    for seg in range(GROUPS):
        from_seg = (even, odd)[seg % 2][:, seg // 2].reshape(chips, 2, 8, LANES)
        for core in range(2):
            rows8 = from_seg[:, core]
            tile = jnp.concatenate(
                [jnp.where(mine == 0, rows8, 0.0), jnp.where(mine == 1, rows8, 0.0)], axis=1
            )
            joined[slots[core], seg * chips : (seg + 1) * chips, part:, :] = tile.astype(BF)

    at_skip = layers * 4 * width * width // LANES
    at_res = at_skip + layers * width * width // LANES
    at_in = at_res + (layers - 1) * width * width // LANES
    at_out = at_in + feat * width // LANES
    end = put_slabs(at_out, dot_at(xs[...], active)[feat:, :])
    put(end, jnp.zeros((joined.shape[0] * half_rows - end, LANES), BF))

    for layer in reversed(range(layers)):
        h = hs[layer]
        lag = TILE * 2**layer
        last = layer == layers - 1
        dg = dot_bt(sd[:, :width], w_skip[layer])
        if not last:
            dg = dg + dot_bt(sd[:, width:], w_res[layer])
        dz[:rows, :width] = (dg * p_all[layer].astype(F32)).astype(BF)
        dz[:rows, width:] = (dg * q_all[layer].astype(F32)).astype(BF)
        gated = g_all[:, layer * width : (layer + 1) * width]
        side = dot_at(gated, sd[:, :width] if last else sd[...])
        put_slabs(at_skip + layer * width * width // LANES, side[:, :width])
        if not last:
            put_slabs(at_res + layer * width * width // LANES, side[:, width:])
        dz[rows : rows + lag] = wrapped(dz[:lag], -4)
        later = dz[lag : lag + rows]
        here = dz[:rows]
        grown = dot_bt(later, w_conv[layer, 0]) + dot_bt(here, w_conv[layer, 1])
        if not last:
            grown = grown + dh[...]
        dh[...] = grown
        sd[:, width:] = grown.astype(BF)
        row = layer * 4 * width * width // LANES
        row = put_slabs(row, dot_at(h[top:, :], later))
        put_slabs(row, dot_at(h[top:, :], here))

    put_slabs(at_in, dot_at(xs[...], sd[:, width:])[:feat, :])
    last_copies = []
    span = joined.shape[1] // SPLIT
    for slot, to in ((1, send_out), (0, keep_out)):
        for at in range(SPLIT):
            some = pl.ds(at * span, span)
            copy = pltpu.make_async_copy(
                joined.at[slot, some], to.at[some], sems.at[6 + layers + slot * SPLIT + at]
            )
            copy.start()
            last_copies.append(copy)
    for copy in last_copies:
        copy.wait()


def local_step(mine, got, w_in, w_conv, w_res, w_skip, w_out, chips, part):
    feat, width = w_in.shape
    layers = w_conv.shape[0]
    rows = got.shape[0] * got.shape[1]
    pad = TILE * 2 ** (layers - 1)
    flops = 2 * rows * width * (layers * (3 * 4 * width + 3 * 2 * width))
    half = jax.ShapeDtypeStruct((chips, part + TILE, LANES), BF)
    return pl.pallas_call(
        functools.partial(step_kernel, layers=layers, width=width, part=part, feat=feat),
        out_shape=(half, half),
        in_specs=[SMEM, VMEM] + [HBM] * 5,
        out_specs=(ANY, ANY),
        scratch_shapes=[
            pltpu.VMEM(w_in.shape, BF),
            pltpu.VMEM(w_conv.shape, BF),
            pltpu.VMEM(w_res.shape, BF),
            pltpu.VMEM(w_skip.shape, BF),
            pltpu.VMEM(w_out.shape[::-1], BF),
            pltpu.VMEM((LANES, 2 * width), BF),
            pltpu.VMEM((2 * LANES, width), BF),
            pltpu.VMEM((rows, LANES), BF),
        ]
        + [pltpu.VMEM((rows + pad, width), BF)] * layers
        + [
            pltpu.VMEM((layers, rows, width), BF),
            pltpu.VMEM((layers, rows, width), BF),
            pltpu.VMEM((rows, layers * width), BF),
            pltpu.VMEM((rows, 2 * width), BF),
            pltpu.VMEM((rows, width), F32),
            pltpu.VMEM((rows + pad, 2 * width), BF),
            pltpu.VMEM((2, chips, part + TILE, LANES), BF),
            pltpu.SemaphoreType.DMA((6 + layers + 2 * SPLIT,)),
        ],
        compiler_params=grant(46),
        cost_estimate=pl.CostEstimate(
            flops=flops, transcendentals=rows * width * 2 * layers, bytes_accessed=2**23
        ),
        name="residue_step",
    )(
        mine,
        got.reshape(GROUPS, -1, TILE, LANES),
        *(pltpu.with_memory_space_constraint(w, pltpu.HBM) for w in (w_in, w_conv, w_res, w_skip, w_out.T)),
    )


def total_kernel(out, spread, pred_t, *, part):
    chips = out.shape[0]
    total = jnp.sum(out[:, :part, :].astype(F32), axis=0).astype(BF)
    for chip in range(chips):
        spread[chip] = total
    rows = out[:, part:, :].astype(F32).reshape(chips, 2, 8, LANES)
    span = chips * 8
    for k, piece in enumerate(merge(rows[:, 0], rows[:, 1])):
        turned = piece.reshape(span, LANES).T
        for half in range(2):
            at = (2 * half + k) * span
            pred_t[:, at : at + span] = turned[half * 64 : half * 64 + 64].astype(BF)


def unpack_kernel(mine_ref, piece, *refs, part, own):
    conv_out, res_out, skip_out, in_out, out_out, conv, res, skip, first, last, sems = refs[-11:]
    low = (mine_ref[0] == 0) if own else (mine_ref[0] == 1)
    cut = piece.shape[0] * part

    def fill(row, to):
        rows, cols = to.shape
        for lane in range(0, cols, LANES):
            at = 0
            while at < rows:
                chip, start = divmod(row + at, part)
                take = min(part - start, rows - at)
                to[at : at + take, lane : lane + LANES] = piece[chip, start : start + take, :].astype(F32)
                at += take
            row += rows
        return row

    def leave(copies, scratch, out):
        copy = pltpu.make_async_copy(scratch, out, sems.at[len(copies)])
        copy.start()
        copies.append(copy)

    layers = conv.shape[0]
    per_layer = 2 * conv.shape[2] * conv.shape[3] // LANES
    low_layers = cut // per_layer
    assert low_layers * per_layer == cut

    @pl.when(low)
    def _():
        copies = []
        row = 0
        for layer in range(low_layers):
            for tap in range(2):
                row = fill(row, conv.at[layer, tap])
            leave(copies, conv.at[layer], conv_out.at[layer])
        for copy in copies:
            copy.wait()

    @pl.when(jnp.logical_not(low))
    def _():
        copies = []
        row = 0
        for layer in range(low_layers, layers):
            for tap in range(2):
                row = fill(row, conv.at[layer, tap])
            leave(copies, conv.at[layer], conv_out.at[layer])
        for kind, out in ((skip, skip_out), (res, res_out)):
            for layer in range(kind.shape[0]):
                row = fill(row, kind.at[layer])
            leave(copies, kind, out)
        for kind, out in ((first, in_out), (last, out_out)):
            row = fill(row, kind)
            leave(copies, kind, out)
        for copy in copies:
            copy.wait()


def unpack(mine, piece, shapes, part, before=()):
    return pl.pallas_call(
        functools.partial(unpack_kernel, part=part, own=not before),
        out_shape=tuple(jax.ShapeDtypeStruct(s, F32) for s in shapes),
        in_specs=[SMEM, VMEM] + [ANY] * len(before),
        out_specs=(ANY,) * len(shapes),
        scratch_shapes=[pltpu.VMEM(s, F32) for s in shapes] + [pltpu.SemaphoreType.DMA((8,))],
        input_output_aliases={2 + k: k for k in range(len(before))},
        compiler_params=grant(12),
        cost_estimate=pl.CostEstimate(flops=2**21, transcendentals=0, bytes_accessed=2**22),
        name="unpack_rest" if before else "unpack_own",
    )(mine, piece, *before)


def body(stream, w_in, w_conv, w_res, w_skip, w_out, grad_pred):
    feat, width = w_in.shape
    rows = stream.shape[0]
    chips = lax.axis_size(CHIPS)
    devices = chips * lax.axis_size("c")
    sent = pl.pallas_call(
        regroup_kernel,
        out_shape=jax.ShapeDtypeStruct((devices, TILE, LANES), BF),
        in_specs=[HBM] * 2,
        out_specs=VMEM,
        scratch_shapes=[pltpu.VMEM((2 * feat, rows), BF), pltpu.SemaphoreType.DMA((2,))],
        compiler_params=grant(8),
        name="regroup",
    )(*(pltpu.with_memory_space_constraint(x.T, pltpu.HBM) for x in (stream, grad_pred)))
    mine, sent = lax.optimization_barrier((lax.axis_index("c")[None], sent))
    got = lax.all_to_all(sent, ALL, 0, 0)
    swap = [(0, 1), (1, 0)]
    filled = (w_conv.size + w_res.size + w_skip.size + w_in.size + w_out.size) // LANES
    part = -(-filled // (devices * TILE)) * TILE
    kept, sent = local_step(mine, got, w_in, w_conv, w_res, w_skip, w_out, chips, part)
    away = lax.ppermute(sent, "c", swap)
    summed = (kept.astype(F32) + away.astype(F32)).astype(BF)
    out = lax.all_to_all(summed, CHIPS, 0, 0)
    spread, pred_t = pl.pallas_call(
        functools.partial(total_kernel, part=part),
        out_shape=(
            jax.ShapeDtypeStruct((chips, part, LANES), BF),
            jax.ShapeDtypeStruct((feat, rows), BF),
        ),
        in_specs=[VMEM],
        out_specs=(VMEM, VMEM),
        compiler_params=grant(10),
        name="total",
    )(out)
    spread = lax.all_to_all(spread, CHIPS, 0, 0)
    theirs = lax.ppermute(spread, "c", swap)
    shapes = [w_conv.shape, w_res.shape, w_skip.shape, w_in.shape, w_out.shape[::-1]]
    own = unpack(mine, spread, shapes, part)
    o_conv, o_res, o_skip, o_in, o_out_t = unpack(mine, theirs, shapes, part, own)
    return pred_t.T, o_in, o_conv, o_res, o_skip, o_out_t.T


def solution(mesh):
    grid = Mesh(mesh.devices.reshape(4, 4, 4, 2), ALL)
    placed = (P(ALL, None), P(), P(), P(), P(), P(), P(ALL, None))
    return jax.shard_map(
        body,
        mesh=grid,
        in_specs=placed,
        out_specs=(P(ALL, None), P(), P(), P(), P(), P()),
        check_vma=False,
    )
```

```python
import functools
import jax
import jax.numpy as jnp
from jax import lax
from jax.experimental import pallas as pl
from jax.experimental.pallas import tpu as pltpu
from jax.sharding import Mesh, PartitionSpec as P

CHIPS = ("x", "y", "z")
ALL = ("x", "y", "z", "c")
BF = jnp.bfloat16
F32 = jnp.float32
LANES = 128
TILE = 16
GROUPS = 4
VMEM = pl.BlockSpec(memory_space=pltpu.VMEM)
SMEM = pl.BlockSpec(memory_space=pltpu.SMEM)
ANY = pl.BlockSpec(memory_space=pl.ANY)
HBM = pl.BlockSpec(memory_space=pltpu.HBM)


def grant(mib):
    return pltpu.CompilerParams(vmem_limit_bytes=mib * 2**20)


def dot(left, right):
    return jnp.dot(left, right, preferred_element_type=F32)


def dot_bt(left, right):
    return lax.dot_general(left, right, (((1,), (1,)), ((), ())), preferred_element_type=F32)


def dot_at(left, right):
    return lax.dot_general(left, right, (((0,), (0,)), ((), ())), preferred_element_type=F32)


def merge(left, right):
    def shift(v, by):
        flat = v.reshape(-1, LANES)
        return pltpu.roll(flat, by % flat.shape[0], 0).reshape(v.shape)

    low = lax.broadcasted_iota(jnp.int32, left.shape, left.ndim - 2) < 4
    return jnp.where(low, left, shift(right, 4)), jnp.where(low, shift(left, -4), right)


def regroup_kernel(stream_t, grad_t, *refs):
    both, sems = refs[-2:]
    count = (len(refs) - 3) // 2
    sent, fetched = refs[count], refs[count + 1 : -2]
    feat = stream_t.shape[0]
    copies = [
        pltpu.make_async_copy(stream_t, both.at[:feat], sems.at[0]),
        pltpu.make_async_copy(grad_t, both.at[feat:], sems.at[1]),
    ]
    fetches = [
        pltpu.make_async_copy(refs[k], fetched[k], sems.at[2 + k]) for k in range(count)
    ]
    for copy in copies + fetches:
        copy.start()
    for copy in copies:
        copy.wait()
    x = both[...].astype(F32).T
    devices = sent.shape[0]
    x = x.reshape(4, devices // 2, 8, LANES)
    halves = []
    for k in range(2):
        even, odd = merge(x[2 * k], x[2 * k + 1])
        halves.append(jnp.stack([even, odd], axis=1))
    sent[...] = jnp.stack(halves, axis=2).reshape(sent.shape).astype(BF)
    for copy in fetches:
        copy.wait()


def step_kernel(
    mine_ref, got, w_in, w_conv, w_res, w_skip, w_out_t, keep_out, send_out,
    w_first, w_wide_t, xs, h0, h1, h2, h3, p_all, q_all, g_all, sd, dh, dz, joined, sems,
    *, layers, width, part, feat,
):
    rows = xs.shape[0]
    steps = rows // (TILE * GROUPS)
    hs = (h0, h1, h2, h3)
    mine = mine_ref[0]
    slots = (mine, 1 - mine)
    half_rows = joined.shape[1] * part
    top = h0.shape[0] - rows

    def put(row, value):
        n, done = value.shape[0], 0
        while done < n:
            half, inside = divmod(row + done, half_rows)
            chip, low = divmod(inside, part)
            take = min(part - low, n - done)
            joined[slots[half], chip, low : low + take, :] = value[done : done + take]
            done += take

    def put_slabs(row, value):
        for lane in range(0, value.shape[1], LANES):
            put(row, value[:, lane : lane + LANES].astype(BF))
            row += value.shape[0]
        return row

    def wrapped(tail, by):
        v = tail.astype(F32)
        v = pltpu.roll(v, by % v.shape[0], 0)
        row = lax.broadcasted_iota(jnp.int32, v.shape, 0) % TILE
        keep = row >= by if by > 0 else row < TILE + by
        return jnp.where(keep, v, 0.0).astype(BF)

    g = [got[s].astype(F32).reshape(steps, 2, 8, LANES) for s in range(GROUPS)]
    pairs = [merge(g[2 * k], g[2 * k + 1]) for k in range(2)]
    even = jnp.stack([pairs[0][0], pairs[1][0]], axis=2)
    odd = jnp.stack([pairs[0][1], pairs[1][1]], axis=2)
    xs[...] = jnp.stack([even, odd], axis=2).reshape(rows, LANES).astype(BF)
    none = jnp.zeros((feat, width), BF)
    w_first[:feat, :width] = w_in[...]
    w_first[feat:, :width] = none
    w_first[:feat, width:] = none
    w_first[feat:, width:] = w_out_t[...]
    w_wide_t[:feat, :] = w_out_t[...]
    w_wide_t[feat : 2 * feat, :] = none
    w_wide_t[2 * feat : 3 * feat, :] = none
    w_wide_t[3 * feat :, :] = w_out_t[...]
    h0[top:, :] = dot(xs[...], w_first[:, :width]).astype(BF)

    for layer in range(layers):
        h = hs[layer]
        lag = TILE * 2**layer
        h[top - lag : top] = wrapped(h[top + rows - lag :], 4)
        here = h[top:, :]
        z = dot(h[top - lag : top - lag + rows, :], w_conv[layer, 0]) + dot(here, w_conv[layer, 1])
        a = jnp.tanh(z[:, :width])
        b = 0.5 * jnp.tanh(0.5 * z[:, width:]) + 0.5
        gate = a * b
        p_all[layer] = (b - a * gate).astype(BF)
        q_all[layer] = (gate - gate * b).astype(BF)
        gated = gate.astype(BF)
        g_all[:, layer * width : (layer + 1) * width] = gated
        if layer < layers - 1:
            hs[layer + 1][top:, :] = (here.astype(F32) + dot(gated, w_res[layer])).astype(BF)

    skip = dot(g_all[...], w_skip[...].reshape(layers * width, width))
    s = 0.5 * jnp.tanh(0.5 * skip) + 0.5
    active = (skip * s).astype(BF)
    sd[:, :width] = (dot(xs[...], w_first[:, width:]) * s * (1.0 + skip * (1.0 - s))).astype(BF)
    both = dot_bt(active, w_wide_t[...])
    pa = both[:, :LANES].reshape(steps, 4, 2, 8, LANES)
    pb = both[:, LANES:].reshape(steps, 4, 2, 8, LANES)
    even, odd = merge(pa[:, 0] + pb[:, 2], pa[:, 1] + pb[:, 3])
    chips = joined.shape[1] // GROUPS
    for seg in range(GROUPS):
        from_seg = (even, odd)[seg % 2][:, seg // 2].reshape(chips, 2, 8, LANES)
        for core in range(2):
            rows8 = from_seg[:, core]
            tile = jnp.concatenate(
                [jnp.where(mine == 0, rows8, 0.0), jnp.where(mine == 1, rows8, 0.0)], axis=1
            )
            joined[slots[core], seg * chips : (seg + 1) * chips, part:, :] = tile.astype(BF)

    at_skip = layers * 4 * width * width // LANES
    at_res = at_skip + layers * width * width // LANES
    at_in = at_res + (layers - 1) * width * width // LANES
    at_out = at_in + feat * width // LANES
    end = put_slabs(at_out, dot_at(xs[...], active)[feat:, :])
    put(end, jnp.zeros((joined.shape[0] * half_rows - end, LANES), BF))

    for layer in reversed(range(layers)):
        h = hs[layer]
        lag = TILE * 2**layer
        last = layer == layers - 1
        dg = dot_bt(sd[:, :width], w_skip[layer])
        if not last:
            dg = dg + dot_bt(sd[:, width:], w_res[layer])
        dz[:rows, :width] = (dg * p_all[layer].astype(F32)).astype(BF)
        dz[:rows, width:] = (dg * q_all[layer].astype(F32)).astype(BF)
        gated = g_all[:, layer * width : (layer + 1) * width]
        side = dot_at(gated, sd[:, :width] if last else sd[...])
        put_slabs(at_skip + layer * width * width // LANES, side[:, :width])
        if not last:
            put_slabs(at_res + layer * width * width // LANES, side[:, width:])
        dz[rows : rows + lag] = wrapped(dz[:lag], -4)
        later = dz[lag : lag + rows]
        here = dz[:rows]
        grown = dot_bt(later, w_conv[layer, 0]) + dot_bt(here, w_conv[layer, 1])
        if not last:
            grown = grown + dh[...]
        dh[...] = grown
        sd[:, width:] = grown.astype(BF)
        row = layer * 4 * width * width // LANES
        row = put_slabs(row, dot_at(h[top:, :], later))
        put_slabs(row, dot_at(h[top:, :], here))

    put_slabs(at_in, dot_at(xs[...], sd[:, width:])[:feat, :])
    send = pltpu.make_async_copy(joined.at[1], send_out, sems.at[0])
    keep = pltpu.make_async_copy(joined.at[0], keep_out, sems.at[1])
    send.start()
    keep.start()
    send.wait()
    keep.wait()


def local_step(mine, got, w_in, w_conv, w_res, w_skip, w_out_t, chips, part):
    feat, width = w_in.shape
    layers = w_conv.shape[0]
    rows = got.shape[0] * got.shape[1]
    pad = TILE * 2 ** (layers - 1)
    flops = 2 * rows * width * (layers * (3 * 4 * width + 3 * 2 * width))
    half = jax.ShapeDtypeStruct((chips, part + TILE, LANES), BF)
    return pl.pallas_call(
        functools.partial(step_kernel, layers=layers, width=width, part=part, feat=feat),
        out_shape=(half, half),
        in_specs=[SMEM] + [VMEM] * 6,
        out_specs=(ANY, ANY),
        scratch_shapes=[
            pltpu.VMEM((LANES, 2 * width), BF),
            pltpu.VMEM((2 * LANES, width), BF),
            pltpu.VMEM((rows, LANES), BF),
        ]
        + [pltpu.VMEM((rows + pad, width), BF)] * layers
        + [
            pltpu.VMEM((layers, rows, width), BF),
            pltpu.VMEM((layers, rows, width), BF),
            pltpu.VMEM((rows, layers * width), BF),
            pltpu.VMEM((rows, 2 * width), BF),
            pltpu.VMEM((rows, width), F32),
            pltpu.VMEM((rows + pad, 2 * width), BF),
            pltpu.VMEM((2, chips, part + TILE, LANES), BF),
            pltpu.SemaphoreType.DMA((2,)),
        ],
        compiler_params=grant(42),
        cost_estimate=pl.CostEstimate(
            flops=flops, transcendentals=rows * width * 2 * layers, bytes_accessed=2**23
        ),
        name="residue_step",
    )(
        mine,
        got.reshape(GROUPS, -1, TILE, LANES),
        w_in,
        w_conv,
        w_res,
        w_skip,
        w_out_t,
    )


def total_kernel(out, spread, pred_t, *, part):
    chips = out.shape[0]
    total = jnp.sum(out[:, :part, :].astype(F32), axis=0).astype(BF)
    for chip in range(chips):
        spread[chip] = total
    rows = out[:, part:, :].astype(F32).reshape(chips, 2, 8, LANES)
    span = chips * 8
    for k, piece in enumerate(merge(rows[:, 0], rows[:, 1])):
        turned = piece.reshape(span, LANES).T
        for half in range(2):
            at = (2 * half + k) * span
            pred_t[:, at : at + span] = turned[half * 64 : half * 64 + 64].astype(BF)


def unpack_kernel(mine_ref, piece, *refs, part, own):
    conv_out, res_out, skip_out, in_out, out_out, conv, res, skip, first, last, sems = refs[-11:]
    low = (mine_ref[0] == 0) if own else (mine_ref[0] == 1)
    cut = piece.shape[0] * part

    def fill(row, to):
        rows, cols = to.shape
        for lane in range(0, cols, LANES):
            at = 0
            while at < rows:
                chip, start = divmod(row + at, part)
                take = min(part - start, rows - at)
                to[at : at + take, lane : lane + LANES] = piece[chip, start : start + take, :].astype(F32)
                at += take
            row += rows
        return row

    def leave(copies, scratch, out):
        copy = pltpu.make_async_copy(scratch, out, sems.at[len(copies)])
        copy.start()
        copies.append(copy)

    layers = conv.shape[0]
    per_layer = 2 * conv.shape[2] * conv.shape[3] // LANES
    low_layers = cut // per_layer
    assert low_layers * per_layer == cut

    @pl.when(low)
    def _():
        copies = []
        row = 0
        for layer in range(low_layers):
            for tap in range(2):
                row = fill(row, conv.at[layer, tap])
            leave(copies, conv.at[layer], conv_out.at[layer])
        for copy in copies:
            copy.wait()

    @pl.when(jnp.logical_not(low))
    def _():
        copies = []
        row = 0
        for layer in range(low_layers, layers):
            for tap in range(2):
                row = fill(row, conv.at[layer, tap])
            leave(copies, conv.at[layer], conv_out.at[layer])
        for kind, out in ((skip, skip_out), (res, res_out)):
            for layer in range(kind.shape[0]):
                row = fill(row, kind.at[layer])
            leave(copies, kind, out)
        for kind, out in ((first, in_out), (last, out_out)):
            row = fill(row, kind)
            leave(copies, kind, out)
        for copy in copies:
            copy.wait()


def unpack(mine, piece, shapes, part, before=()):
    return pl.pallas_call(
        functools.partial(unpack_kernel, part=part, own=not before),
        out_shape=tuple(jax.ShapeDtypeStruct(s, F32) for s in shapes),
        in_specs=[SMEM, VMEM] + [ANY] * len(before),
        out_specs=(ANY,) * len(shapes),
        scratch_shapes=[pltpu.VMEM(s, F32) for s in shapes] + [pltpu.SemaphoreType.DMA((8,))],
        input_output_aliases={2 + k: k for k in range(len(before))},
        compiler_params=grant(12),
        cost_estimate=pl.CostEstimate(flops=2**21, transcendentals=0, bytes_accessed=2**22),
        name="unpack_rest" if before else "unpack_own",
    )(mine, piece, *before)


def body(stream, w_in, w_conv, w_res, w_skip, w_out, grad_pred):
    feat, width = w_in.shape
    rows = stream.shape[0]
    chips = lax.axis_size(CHIPS)
    devices = chips * lax.axis_size("c")
    weights = (w_in, w_conv, w_res, w_skip, w_out.T)
    sources = (stream.T, grad_pred.T, *weights)
    sent, *weights = pl.pallas_call(
        regroup_kernel,
        out_shape=(
            jax.ShapeDtypeStruct((devices, TILE, LANES), BF),
            *(jax.ShapeDtypeStruct(w.shape, BF) for w in weights),
        ),
        in_specs=[HBM] * len(sources),
        out_specs=(VMEM, *(ANY for _ in weights)),
        scratch_shapes=[
            pltpu.VMEM((2 * feat, rows), BF),
            pltpu.SemaphoreType.DMA((len(sources),)),
        ],
        compiler_params=grant(8),
        name="regroup",
    )(*(pltpu.with_memory_space_constraint(x, pltpu.HBM) for x in sources))
    mine, sent = lax.optimization_barrier((lax.axis_index("c")[None], sent))
    got = lax.all_to_all(sent, ALL, 0, 0)
    swap = [(0, 1), (1, 0)]
    filled = (w_conv.size + w_res.size + w_skip.size + w_in.size + w_out.size) // LANES
    part = -(-filled // (devices * TILE)) * TILE
    kept, sent = local_step(mine, got, *weights, chips, part)
    away = lax.ppermute(sent, "c", swap)
    summed = (kept.astype(F32) + away.astype(F32)).astype(BF)
    out = lax.all_to_all(summed, CHIPS, 0, 0)
    spread, pred_t = pl.pallas_call(
        functools.partial(total_kernel, part=part),
        out_shape=(
            jax.ShapeDtypeStruct((chips, part, LANES), BF),
            jax.ShapeDtypeStruct((feat, rows), BF),
        ),
        in_specs=[VMEM],
        out_specs=(VMEM, VMEM),
        compiler_params=grant(10),
        name="total",
    )(out)
    spread = lax.all_to_all(spread, CHIPS, 0, 0)
    theirs = lax.ppermute(spread, "c", swap)
    shapes = [w_conv.shape, w_res.shape, w_skip.shape, w_in.shape, w_out.shape[::-1]]
    own = unpack(mine, spread, shapes, part)
    o_conv, o_res, o_skip, o_in, o_out_t = unpack(mine, theirs, shapes, part, own)
    return pred_t.T, o_in, o_conv, o_res, o_skip, o_out_t.T


def solution(mesh):
    grid = Mesh(mesh.devices.reshape(4, 4, 4, 2), ALL)
    placed = (P(ALL, None), P(), P(), P(), P(), P(), P(ALL, None))
    return jax.shard_map(
        body,
        mesh=grid,
        in_specs=placed,
        out_specs=(P(ALL, None), P(), P(), P(), P(), P()),
        check_vma=False,
    )
```

```python
import functools
import jax
import jax.numpy as jnp
from jax import lax
from jax.experimental import pallas as pl
from jax.experimental.pallas import tpu as pltpu
from jax.sharding import Mesh, PartitionSpec as P

CHIPS = ("x", "y", "z")
ALL = ("x", "y", "z", "c")
BF = jnp.bfloat16
F32 = jnp.float32
LANES = 128
TILE = 16
GROUPS = 4
VMEM = pl.BlockSpec(memory_space=pltpu.VMEM)
SMEM = pl.BlockSpec(memory_space=pltpu.SMEM)
ANY = pl.BlockSpec(memory_space=pl.ANY)
HBM = pl.BlockSpec(memory_space=pltpu.HBM)


def grant(mib):
    return pltpu.CompilerParams(vmem_limit_bytes=mib * 2**20)


def dot(left, right):
    return jnp.dot(left, right, preferred_element_type=F32)


def dot_bt(left, right):
    return lax.dot_general(left, right, (((1,), (1,)), ((), ())), preferred_element_type=F32)


def dot_at(left, right):
    return lax.dot_general(left, right, (((0,), (0,)), ((), ())), preferred_element_type=F32)


def merge(left, right):
    def shift(v, by):
        flat = v.reshape(-1, LANES)
        return pltpu.roll(flat, by % flat.shape[0], 0).reshape(v.shape)

    low = lax.broadcasted_iota(jnp.int32, left.shape, left.ndim - 2) < 4
    return jnp.where(low, left, shift(right, 4)), jnp.where(low, shift(left, -4), right)


def regroup_kernel(stream_t, grad_t, *refs):
    both, sems = refs[-2:]
    count = (len(refs) - 3) // 2
    sent, fetched = refs[count], refs[count + 1 : -2]
    feat = stream_t.shape[0]
    copies = [
        pltpu.make_async_copy(stream_t, both.at[:feat], sems.at[0]),
        pltpu.make_async_copy(grad_t, both.at[feat:], sems.at[1]),
    ]
    fetches = [
        pltpu.make_async_copy(refs[k], fetched[k], sems.at[2 + k]) for k in range(count)
    ]
    for copy in copies + fetches:
        copy.start()
    for copy in copies:
        copy.wait()
    x = both[...].astype(F32).T
    devices = sent.shape[0]
    x = x.reshape(4, devices // 2, 8, LANES)
    halves = []
    for k in range(2):
        even, odd = merge(x[2 * k], x[2 * k + 1])
        halves.append(jnp.stack([even, odd], axis=1))
    sent[...] = jnp.stack(halves, axis=2).reshape(sent.shape).astype(BF)
    for copy in fetches:
        copy.wait()


def step_kernel(
    mine_ref, got, w_in, w_conv, w_res, w_skip, w_out_t, keep_out, send_out,
    w_first, w_wide_t, xs, h0, h1, h2, h3, p_all, q_all, g_all, sd, dh, dz, joined, sems,
    *, layers, width, part, feat,
):
    rows = xs.shape[0]
    steps = rows // (TILE * GROUPS)
    hs = (h0, h1, h2, h3)
    mine = mine_ref[0]
    slots = (mine, 1 - mine)
    half_rows = joined.shape[1] * part
    top = h0.shape[0] - rows

    def put(row, value):
        n, done = value.shape[0], 0
        while done < n:
            half, inside = divmod(row + done, half_rows)
            chip, low = divmod(inside, part)
            take = min(part - low, n - done)
            joined[slots[half], chip, low : low + take, :] = value[done : done + take]
            done += take

    def put_slabs(row, value):
        for lane in range(0, value.shape[1], LANES):
            put(row, value[:, lane : lane + LANES].astype(BF))
            row += value.shape[0]
        return row

    def wrapped(tail, by):
        v = tail.astype(F32)
        v = pltpu.roll(v, by % v.shape[0], 0)
        row = lax.broadcasted_iota(jnp.int32, v.shape, 0) % TILE
        keep = row >= by if by > 0 else row < TILE + by
        return jnp.where(keep, v, 0.0).astype(BF)

    g = [got[s].astype(F32).reshape(steps, 2, 8, LANES) for s in range(GROUPS)]
    pairs = [merge(g[2 * k], g[2 * k + 1]) for k in range(2)]
    even = jnp.stack([pairs[0][0], pairs[1][0]], axis=2)
    odd = jnp.stack([pairs[0][1], pairs[1][1]], axis=2)
    xs[...] = jnp.stack([even, odd], axis=2).reshape(rows, LANES).astype(BF)
    none = jnp.zeros((feat, width), BF)
    w_first[:feat, :width] = w_in[...]
    w_first[feat:, :width] = none
    w_first[:feat, width:] = none
    w_first[feat:, width:] = w_out_t[...]
    w_wide_t[:feat, :] = w_out_t[...]
    w_wide_t[feat : 2 * feat, :] = none
    w_wide_t[2 * feat : 3 * feat, :] = none
    w_wide_t[3 * feat :, :] = w_out_t[...]
    h0[top:, :] = dot(xs[...], w_first[:, :width]).astype(BF)

    for layer in range(layers):
        h = hs[layer]
        lag = TILE * 2**layer
        h[top - lag : top] = wrapped(h[top + rows - lag :], 4)
        here = h[top:, :]
        z = dot(h[top - lag : top - lag + rows, :], w_conv[layer, 0]) + dot(here, w_conv[layer, 1])
        a = jnp.tanh(z[:, :width])
        b = 0.5 * jnp.tanh(0.5 * z[:, width:]) + 0.5
        gate = a * b
        p_all[layer] = (b - a * gate).astype(BF)
        q_all[layer] = (gate - gate * b).astype(BF)
        gated = gate.astype(BF)
        g_all[:, layer * width : (layer + 1) * width] = gated
        if layer < layers - 1:
            hs[layer + 1][top:, :] = (here.astype(F32) + dot(gated, w_res[layer])).astype(BF)

    skip = dot(g_all[...], w_skip[...].reshape(layers * width, width))
    s = 0.5 * jnp.tanh(0.5 * skip) + 0.5
    active = (skip * s).astype(BF)
    sd[:, :width] = (dot(xs[...], w_first[:, width:]) * s * (1.0 + skip * (1.0 - s))).astype(BF)
    both = dot_bt(active, w_wide_t[...])
    pa = both[:, :LANES].reshape(steps, 4, 2, 8, LANES)
    pb = both[:, LANES:].reshape(steps, 4, 2, 8, LANES)
    even, odd = merge(pa[:, 0] + pb[:, 2], pa[:, 1] + pb[:, 3])
    chips = joined.shape[1] // GROUPS
    for seg in range(GROUPS):
        from_seg = (even, odd)[seg % 2][:, seg // 2].reshape(chips, 2, 8, LANES)
        for core in range(2):
            rows8 = from_seg[:, core]
            tile = jnp.concatenate(
                [jnp.where(mine == 0, rows8, 0.0), jnp.where(mine == 1, rows8, 0.0)], axis=1
            )
            joined[slots[core], seg * chips : (seg + 1) * chips, part:, :] = tile.astype(BF)

    at_skip = layers * 4 * width * width // LANES
    at_res = at_skip + layers * width * width // LANES
    at_in = at_res + (layers - 1) * width * width // LANES
    at_out = at_in + feat * width // LANES
    end = put_slabs(at_out, dot_at(xs[...], active)[feat:, :])
    put(end, jnp.zeros((joined.shape[0] * half_rows - end, LANES), BF))

    for layer in reversed(range(layers)):
        h = hs[layer]
        lag = TILE * 2**layer
        last = layer == layers - 1
        dg = dot_bt(sd[:, :width], w_skip[layer])
        if not last:
            dg = dg + dot_bt(sd[:, width:], w_res[layer])
        dz[:rows, :width] = (dg * p_all[layer].astype(F32)).astype(BF)
        dz[:rows, width:] = (dg * q_all[layer].astype(F32)).astype(BF)
        gated = g_all[:, layer * width : (layer + 1) * width]
        side = dot_at(gated, sd[:, :width] if last else sd[...])
        put_slabs(at_skip + layer * width * width // LANES, side[:, :width])
        if not last:
            put_slabs(at_res + layer * width * width // LANES, side[:, width:])
        dz[rows : rows + lag] = wrapped(dz[:lag], -4)
        later = dz[lag : lag + rows]
        here = dz[:rows]
        grown = dot_bt(later, w_conv[layer, 0]) + dot_bt(here, w_conv[layer, 1])
        if not last:
            grown = grown + dh[...]
        dh[...] = grown
        sd[:, width:] = grown.astype(BF)
        row = layer * 4 * width * width // LANES
        row = put_slabs(row, dot_at(h[top:, :], later))
        put_slabs(row, dot_at(h[top:, :], here))

    put_slabs(at_in, dot_at(xs[...], sd[:, width:])[:feat, :])
    send = pltpu.make_async_copy(joined.at[1], send_out, sems.at[0])
    keep = pltpu.make_async_copy(joined.at[0], keep_out, sems.at[1])
    send.start()
    keep.start()
    send.wait()
    keep.wait()


def local_step(mine, got, w_in, w_conv, w_res, w_skip, w_out_t, chips, part):
    feat, width = w_in.shape
    layers = w_conv.shape[0]
    rows = got.shape[0] * got.shape[1]
    pad = TILE * 2 ** (layers - 1)
    flops = 2 * rows * width * (layers * (3 * 4 * width + 3 * 2 * width))
    half = jax.ShapeDtypeStruct((chips, part + TILE, LANES), BF)
    return pl.pallas_call(
        functools.partial(step_kernel, layers=layers, width=width, part=part, feat=feat),
        out_shape=(half, half),
        in_specs=[SMEM] + [VMEM] * 6,
        out_specs=(ANY, ANY),
        scratch_shapes=[
            pltpu.VMEM((LANES, 2 * width), BF),
            pltpu.VMEM((2 * LANES, width), BF),
            pltpu.VMEM((rows, LANES), BF),
        ]
        + [pltpu.VMEM((rows + pad, width), BF)] * layers
        + [
            pltpu.VMEM((layers, rows, width), BF),
            pltpu.VMEM((layers, rows, width), BF),
            pltpu.VMEM((rows, layers * width), BF),
            pltpu.VMEM((rows, 2 * width), BF),
            pltpu.VMEM((rows, width), F32),
            pltpu.VMEM((rows + pad, 2 * width), BF),
            pltpu.VMEM((2, chips, part + TILE, LANES), BF),
            pltpu.SemaphoreType.DMA((2,)),
        ],
        compiler_params=grant(42),
        cost_estimate=pl.CostEstimate(
            flops=flops, transcendentals=rows * width * 2 * layers, bytes_accessed=2**23
        ),
        name="residue_step",
    )(
        mine,
        got.reshape(GROUPS, -1, TILE, LANES),
        w_in,
        w_conv,
        w_res,
        w_skip,
        w_out_t,
    )


def total_kernel(out, spread, *, part):
    chips = out.shape[0]
    total = jnp.sum(out[:, :part, :].astype(F32), axis=0).astype(BF)
    for chip in range(chips):
        spread[chip] = total


def place_prediction(out, pred_t, part):
    chips = out.shape[0]
    rows = out[:, part:, :].astype(F32).reshape(chips, 2, 8, LANES)
    span = chips * 8
    for k, piece in enumerate(merge(rows[:, 0], rows[:, 1])):
        turned = piece.reshape(span, LANES).T
        for half in range(2):
            at = (2 * half + k) * span
            pred_t[:, at : at + span] = turned[half * 64 : half * 64 + 64].astype(BF)


def unpack_kernel(mine_ref, piece, *refs, part, own):
    if own:
        place_prediction(refs[0], refs[6], part)
        refs = refs[:6] + refs[7:]
    conv_out, res_out, skip_out, in_out, out_out, conv, res, skip, first, last, sems = refs[-11:]
    low = (mine_ref[0] == 0) if own else (mine_ref[0] == 1)
    cut = piece.shape[0] * part

    def fill(row, to):
        rows, cols = to.shape
        for lane in range(0, cols, LANES):
            at = 0
            while at < rows:
                chip, start = divmod(row + at, part)
                take = min(part - start, rows - at)
                to[at : at + take, lane : lane + LANES] = piece[chip, start : start + take, :].astype(F32)
                at += take
            row += rows
        return row

    def leave(copies, scratch, out):
        copy = pltpu.make_async_copy(scratch, out, sems.at[len(copies)])
        copy.start()
        copies.append(copy)

    layers = conv.shape[0]
    per_layer = 2 * conv.shape[2] * conv.shape[3] // LANES
    low_layers = cut // per_layer
    assert low_layers * per_layer == cut

    @pl.when(low)
    def _():
        copies = []
        row = 0
        for layer in range(low_layers):
            for tap in range(2):
                row = fill(row, conv.at[layer, tap])
            leave(copies, conv.at[layer], conv_out.at[layer])
        for copy in copies:
            copy.wait()

    @pl.when(jnp.logical_not(low))
    def _():
        copies = []
        row = 0
        for layer in range(low_layers, layers):
            for tap in range(2):
                row = fill(row, conv.at[layer, tap])
            leave(copies, conv.at[layer], conv_out.at[layer])
        for kind, out in ((skip, skip_out), (res, res_out)):
            for layer in range(kind.shape[0]):
                row = fill(row, kind.at[layer])
            leave(copies, kind, out)
        for kind, out in ((first, in_out), (last, out_out)):
            row = fill(row, kind)
            leave(copies, kind, out)
        for copy in copies:
            copy.wait()


def unpack(mine, piece, shapes, part, before=(), received=(), pred=()):
    return pl.pallas_call(
        functools.partial(unpack_kernel, part=part, own=not before),
        out_shape=tuple(jax.ShapeDtypeStruct(s, F32) for s in shapes) + pred,
        in_specs=[SMEM, VMEM] + [VMEM] * len(received) + [ANY] * len(before),
        out_specs=(ANY,) * len(shapes) + (VMEM,) * len(pred),
        scratch_shapes=[pltpu.VMEM(s, F32) for s in shapes] + [pltpu.SemaphoreType.DMA((8,))],
        input_output_aliases={2 + k: k for k in range(len(before))},
        compiler_params=grant(12),
        cost_estimate=pl.CostEstimate(flops=2**21, transcendentals=0, bytes_accessed=2**22),
        name="unpack_rest" if before else "unpack_own",
    )(mine, piece, *received, *before)


def body(stream, w_in, w_conv, w_res, w_skip, w_out, grad_pred):
    feat, width = w_in.shape
    rows = stream.shape[0]
    chips = lax.axis_size(CHIPS)
    devices = chips * lax.axis_size("c")
    weights = (w_in, w_conv, w_res, w_skip, w_out.T)
    sources = (stream.T, grad_pred.T, *weights)
    sent, *weights = pl.pallas_call(
        regroup_kernel,
        out_shape=(
            jax.ShapeDtypeStruct((devices, TILE, LANES), BF),
            *(jax.ShapeDtypeStruct(w.shape, BF) for w in weights),
        ),
        in_specs=[HBM] * len(sources),
        out_specs=(VMEM, *(ANY for _ in weights)),
        scratch_shapes=[
            pltpu.VMEM((2 * feat, rows), BF),
            pltpu.SemaphoreType.DMA((len(sources),)),
        ],
        compiler_params=grant(8),
        name="regroup",
    )(*(pltpu.with_memory_space_constraint(x, pltpu.HBM) for x in sources))
    mine, sent = lax.optimization_barrier((lax.axis_index("c")[None], sent))
    got = lax.all_to_all(sent, ALL, 0, 0)
    swap = [(0, 1), (1, 0)]
    filled = (w_conv.size + w_res.size + w_skip.size + w_in.size + w_out.size) // LANES
    part = -(-filled // (devices * TILE)) * TILE
    kept, sent = local_step(mine, got, *weights, chips, part)
    away = lax.ppermute(sent, "c", swap)
    summed = (kept.astype(F32) + away.astype(F32)).astype(BF)
    out = lax.all_to_all(summed, CHIPS, 0, 0)
    spread = pl.pallas_call(
        functools.partial(total_kernel, part=part),
        out_shape=jax.ShapeDtypeStruct((chips, part, LANES), BF),
        in_specs=[VMEM],
        out_specs=VMEM,
        compiler_params=grant(10),
        name="total",
    )(out)
    spread = lax.all_to_all(spread, CHIPS, 0, 0)
    theirs = lax.ppermute(spread, "c", swap)
    shapes = [w_conv.shape, w_res.shape, w_skip.shape, w_in.shape, w_out.shape[::-1]]
    pred = (jax.ShapeDtypeStruct((feat, rows), BF),)
    *own, pred_t = unpack(mine, spread, shapes, part, received=(out,), pred=pred)
    o_conv, o_res, o_skip, o_in, o_out_t = unpack(mine, theirs, shapes, part, own)
    return pred_t.T, o_in, o_conv, o_res, o_skip, o_out_t.T


def solution(mesh):
    grid = Mesh(mesh.devices.reshape(4, 4, 4, 2), ALL)
    placed = (P(ALL, None), P(), P(), P(), P(), P(), P(ALL, None))
    return jax.shard_map(
        body,
        mesh=grid,
        in_specs=placed,
        out_specs=(P(ALL, None), P(), P(), P(), P(), P()),
        check_vma=False,
    )
```
